32 devices in a mesh: gx: 4 (over z), gy: 4 (over y, x), gz: 2 (over core).
Axes of the slice: x: 2, y: 2, z: 4, core: 2. Of those that a mesh axis runs over, the one named last changes fastest.
Arguments:
- factor_inv: bfloat16 [4, 4096, 2048], P('gx', 'gy', 'gz')
- sep_sizes: int32 [4, 4, 2], P('gx', 'gy', 'gz'), may hold values from 512 to 1024
- coupling: bfloat16 [12, 4096, 2048], P('gx', 'gy', 'gz'), may hold values from -0.109375 to 0.109375
Outputs:
- schur_update: float32 [4, 4096, 2048], P('gx', 'gy', 'gz')
The draws below stay inside these ranges and needn't reach their ends.
All inputs are finite; a program needn't handle non-finite values.
Results may differ from the reference program's by a relative error of at most 0.0023.
Values may be sent and summed in bfloat16 or wider, within the bound.
A program may use at most 128 MiB of HBM per device.

```python
import jax
import jax.numpy as jnp
from jax import lax

W = 1024
M = 1024
SLOTS = 3
N_GX = 4
N_GY = 4
N_GZ = 2


def draw_factor_inv(key, part):
    first, second = jax.random.split(jax.random.fold_in(key, 11))
    shape = (N_GX, N_GY * W, N_GZ * W)
    rows = lax.broadcasted_iota(jnp.int32, shape, 1) % W
    cols = lax.broadcasted_iota(jnp.int32, shape, 2) % W
    lower = jax.random.normal(first, shape, jnp.float32)
    diag = jax.random.uniform(second, shape, jnp.float32, 0.5, 1.5)
    scaled = lower / jnp.sqrt(jnp.float32(W))
    return jnp.where(rows > cols, scaled, jnp.where(rows == cols, diag, jnp.float32(0.0))).astype(jnp.bfloat16)


def with_ends(entries, key, smallest, high):
    shape = entries.shape
    index_at = [jax.random.randint(jax.random.fold_in(key, axis), (), 0, shape[axis]) for axis in range(len(shape))]
    entries = entries.at[tuple(index_at)].set(smallest)
    longest = shape.index(max(shape))
    index_at[longest] = (index_at[longest] + 1) % shape[longest]
    return entries.at[tuple(index_at)].set(high)


def level_of(own_key, extent, cuts, low, largest):
    def one(dim, blocks):
        steps = jax.random.uniform(jax.random.fold_in(jax.random.fold_in(own_key, 6), dim), (blocks,), jnp.float32, low / len(cuts), largest / len(cuts))
        return jnp.repeat(jnp.exp(steps), extent[dim] // blocks).reshape((-1,) + (1,) * (len(extent) - dim - 1))

    gain = one(*cuts[0])
    for cut in cuts[1:]:
        gain = gain * one(*cut)
    return gain


def gaussian(key, dims, spread, most, cuts=(), held_as=jnp.bfloat16):
    drawn = jax.random.normal(key, dims, jnp.float32) * spread
    if len(cuts) > 0:
        drawn = level_of(key, dims, cuts, -0.22, 0.18) * drawn
    return jnp.clip(drawn, min=-most, max=most).astype(held_as)


def setup_inputs(seed: int = 0) -> dict:
    splits = jax.random.split(jax.random.key(seed), 4)
    factor_inv = draw_factor_inv(jax.random.fold_in(splits[3], 71), 0)
    sep_sizes = with_ends(jax.random.randint(splits[1], (N_GX, N_GY, N_GZ), W // 2, W + 1), jax.random.fold_in(splits[1], 1), W // 2, W).astype(jnp.int32)
    coupling = gaussian(splits[2], (N_GX * SLOTS, N_GY * W, N_GZ * M), (3 * W) ** -0.5, 0.109375, ((0, 4), (1, 4), (2, 2)))
    return dict(factor_inv=factor_inv, sep_sizes=sep_sizes, coupling=coupling)


def reference(factor_inv, sep_sizes, coupling):
    nxa = factor_inv.shape[0]
    nya = factor_inv.shape[1] // W
    nza = factor_inv.shape[2] // W
    inner = jnp.arange(W, dtype=jnp.int32)

    def owned(iidx, jidx, kidx):
        valid = (jidx >= 0) & (jidx < nya) & (kidx >= 0) & (kidx < nza)
        jc = jnp.clip(jidx, 0, nya - 1).astype(jnp.int32)
        kc = jnp.clip(kidx, 0, nza - 1).astype(jnp.int32)
        block = lax.dynamic_slice(factor_inv, (iidx, jc * W, kc * W), (1, W, W))[0]
        count = lax.dynamic_slice(sep_sizes, (iidx, jc, kc), (1, 1, 1))[0, 0, 0]
        keep = ((inner < count) & valid).astype(jnp.bfloat16)
        return block * keep[:, None] * keep[None, :]

    def one(flat):
        iidx = (flat // (nya * nza)).astype(jnp.int32)
        jidx = ((flat // nza) % nya).astype(jnp.int32)
        kidx = (flat % nza).astype(jnp.int32)
        cblock = lax.dynamic_slice(coupling, (iidx * 3, jidx * W, kidx * M), (3, W, M))
        factors = [owned(iidx, jidx, kidx - 1), owned(iidx, jidx, kidx + 1), owned(iidx, jidx - 1, kidx)]
        total = jnp.zeros((M, M), jnp.float32)
        for slot in range(3):
            solved = jnp.dot(factors[slot], cblock[slot], preferred_element_type=jnp.float32).astype(jnp.bfloat16)
            total = total + jnp.dot(solved.T, solved, preferred_element_type=jnp.float32)
        return total

    result = lax.map(one, jnp.arange(nxa * nya * nza, dtype=jnp.int32))
    result = result.reshape(nxa, nya, nza, M, M).transpose(0, 1, 3, 2, 4)
    return result.reshape(nxa, nya * M, nza * M)
```

```python
import functools

import jax
import jax.numpy as jnp
from jax import lax
from jax.experimental import pallas as pl
from jax.experimental.pallas import tpu as pltpu
from jax.sharding import PartitionSpec as P

MESH = pl.DeviceIdType.MESH
F32, BF16 = jnp.float32, jnp.bfloat16
LANES = 128
TAIL = 128


def dot(lhs, rhs, left, right):
    return lax.dot_general(lhs, rhs, (((left,), (right,)), ((), ())), preferred_element_type=F32)


def grid_of(rows, cols):
    return (
        lax.broadcasted_iota(jnp.int32, (rows, cols), 0),
        lax.broadcasted_iota(jnp.int32, (rows, cols), 1),
    )


def gather_kernel(
    ny, nz, pieces,
    sizes, factor, coupling,
    total, mine, tail,
    own, couple, beside, solved, mixed, extra, cross, mixed_in, extra_in, cross_in, full,
    load_sem, z_send, z_recv, y_send, y_recv,
):
    width = own.shape[0]
    half = width // 2
    block = half // 2
    steps = width // block
    per = half // LANES
    b, c = lax.axis_index("gy"), lax.axis_index("gz")
    above, below = b < ny - 1, b > 0
    ups, downs = c < nz - 1, c > 0
    peers = ((above, {"gy": b + 1}), (below, {"gy": b - 1}), (ups, {"gz": c + 1}), (downs, {"gz": c - 1}))

    rows_of = [pl.ds(s * block, block) for s in range(steps)]
    factors = [pltpu.make_async_copy(factor.at[0, at], own.at[at], load_sem.at[3 + s]) for s, at in enumerate(rows_of)]
    for load in factors:
        load.start()

    barrier = pltpu.get_barrier_semaphore()
    for there, peer in peers:
        @pl.when(there)
        def _():
            pl.semaphore_signal(barrier, inc=1, device_id=peer, device_id_type=MESH)

    if nz == 2:
        z_loads = [pltpu.make_async_copy(coupling.at[1 - c], couple.at[0], load_sem.at[0])]
    else:
        z_loads = [pltpu.make_async_copy(coupling.at[e], couple.at[e], load_sem.at[e]) for e in range(2)]
    loads = z_loads + [pltpu.make_async_copy(coupling.at[2], mine, load_sem.at[2])]

    size = sizes[0, 0, 0]
    column = (lax.broadcasted_iota(jnp.int32, (1, width), 1) < size).astype(F32).astype(BF16)
    for s in range(steps):
        rows = rows_of[s]
        row = (lax.broadcasted_iota(jnp.int32, (block, 1), 0) + s * block < size).astype(F32).astype(BF16)
        factors[s].wait()
        own[rows, :] = own[rows, :] * row * column

    for load in loads:
        load.start()

    z_copies = []
    for k, (goes, to, comes) in enumerate(((ups, c + 1, downs), (downs, c - 1, ups))):
        copy = pltpu.make_async_remote_copy(
            src_ref=own, dst_ref=beside.at[k if nz > 2 else 0], send_sem=z_send.at[k], recv_sem=z_recv.at[k],
            device_id={"gz": to}, device_id_type=MESH,
        )
        z_copies.append((goes, comes, copy))

    def y_copy(src, dst, k):
        return pltpu.make_async_remote_copy(
            src_ref=src, dst_ref=dst, send_sem=y_send.at[k], recv_sem=y_recv.at[k],
            device_id={"gy": b + 1}, device_id_type=MESH,
        )

    tops = [pl.ds(s * block, block) for s in range(2)]
    mixes = [y_copy(mixed.at[at], mixed_in.at[at], s) for s, at in enumerate(tops)]
    mixes.append(y_copy(extra, extra_in, 2))
    crosses = []
    for k, (start, count) in enumerate(pieces):
        rows = pl.ds(start, count)
        dst = cross_in.at[rows] if k < len(pieces) - 1 else tail
        crosses.append(y_copy(cross.at[rows], dst, k + 3))

    def make_cross(k):
        start, count = pieces[k]
        cross[pl.ds(start, count), :] = dot(own[:, pl.ds(start, count)], own[:, half:], 0, 0).astype(BF16)

    @pl.when(above)
    def _():
        make_cross(0)

    pl.semaphore_wait(barrier, sum(there.astype(jnp.int32) for there, _ in peers))

    @pl.when(above)
    def _():
        crosses[0].start()

    for goes, comes, copy in z_copies:
        @pl.when(goes)
        def _():
            copy.start()

    @pl.when(above)
    def _():
        r, q = grid_of(block, block)
        lines = []
        first = dot(own[:, :block], own[:, :half], 0, 0)
        second = dot(own[:, half : half + block], own[:, half : half + block], 0, 0)
        mixed[:block, :block] = jnp.where(r <= q, first[:, :block], second).astype(BF16)
        mixed[:block, block:] = first[:, block:].astype(BF16)
        mixes[0].start()
        lines.append((first[:, :block], second))
        second = dot(own[:, half + block :], own[:, half:], 0, 0)
        first = dot(own[:, block:half], own[:, block:half], 0, 0)
        mixed[block:, :block] = second[:, :block].astype(BF16)
        mixed[block:, block:] = jnp.where(r <= q, first, second[:, block:]).astype(BF16)
        mixes[1].start()
        lines.append((first, second[:, block:]))
        at = lax.broadcasted_iota(jnp.int32, extra.shape, 0)
        filled = jnp.zeros(extra.shape, F32)
        for s, pair in enumerate(lines):
            one, two = (jnp.sum(jnp.where(r == q, value, 0.0), axis=0, keepdims=True) for value in pair)
            high = two.astype(BF16).astype(F32)
            for group, line in enumerate((high, one - one.astype(BF16).astype(F32), two - high)):
                for i in range(block // LANES):
                    place = group * per + s * (block // LANES) + i
                    filled = jnp.where(at == place, line[:, i * LANES : (i + 1) * LANES], filled)
        extra[...] = filled.astype(BF16)
        mixes[2].start()
        for k in range(1, len(pieces)):
            make_cross(k)
            crosses[k].start()

    for load in loads:
        load.wait()

    def z_slot(slot, k, fresh):
        @pl.loop(0, steps)
        def _(s):
            at = pl.ds(pl.multiple_of(s * block, block), block)
            solved[at, :] = dot(couple[slot, :, at], beside[k], 0, 1).astype(BF16)

        @pl.loop(0, steps)
        def _(s):
            at = pl.ds(pl.multiple_of(s * block, block), block)
            term = dot(solved[at, :], solved[...], 1, 1)
            total[at, :] = term if fresh else total[at, :] + term

    if nz == 2:
        for goes, comes, copy in z_copies:
            @pl.when(comes)
            def _():
                copy.wait_recv()
        z_slot(0, 0, True)
    else:
        total[...] = jnp.zeros_like(total)
        for k, (goes, comes, copy) in enumerate(z_copies):
            @pl.when(comes)
            def _():
                copy.wait_recv()
                z_slot(k, k, False)

    @pl.when(below)
    def _():
        def use_cross(k):
            start, count = pieces[k]
            crosses[k].wait_recv()
            high = dot(cross_in[pl.ds(start, count), :], mine[half:, :], 1, 0).astype(BF16)
            own_rows = mine[pl.ds(start, count), :]
            for i, value in enumerate((own_rows, high, own_rows)):
                solved[pl.ds(i * count, count), :] = value

            @pl.loop(0, steps)
            def _(s):
                at = pl.ds(pl.multiple_of(s * block, block), block)
                term = dot(solved[pl.ds(0, 2 * count), at], solved[pl.ds(count, 2 * count), :], 0, 0)
                total[at, :] = total[at, :] + term

        use_cross(0)
        for copy in mixes:
            copy.wait_recv()
        r, q = grid_of(half, half)
        value = mixed_in[...].astype(F32)
        turned = value.T
        extras = extra_in[...].astype(F32)

        def line(group):
            return jnp.concatenate([extras[group * per + i : group * per + i + 1, :] for i in range(per)], axis=1)

        full[0] = jnp.where(r <= q, value, turned).astype(BF16)
        full[1] = jnp.where(r > q, value, jnp.where(r == q, line(0), turned)).astype(BF16)
        for i in range(2):
            low = jnp.sum(jnp.where(r == q, line(1 + i), 0.0), axis=1, keepdims=True)
            rows = pl.ds(i * half, half)
            piece = mine[rows, :]
            solved[rows, :] = (dot(full[i], piece, 1, 0) + low * piece.astype(F32)).astype(BF16)

        @pl.loop(0, steps)
        def _(s):
            at = pl.ds(pl.multiple_of(s * block, block), block)
            total[at, :] = total[at, :] + dot(mine[:, at], solved[...], 0, 0)

        for k in range(1, len(pieces) - 1):
            use_cross(k)
        crosses[-1].wait_recv()

    for goes, comes, copy in z_copies:
        @pl.when(goes)
        def _():
            copy.wait_send()

    @pl.when(above)
    def _():
        for copy in mixes + crosses:
            copy.wait_send()


def finish_kernel(total, mine, tail, out, left, right, held, store_sem):
    count, half = tail.shape
    width = total.shape[0]
    last = tail.shape[1] - count
    chunk = TAIL

    kept = jnp.where(lax.axis_index("gy") > 0, tail[...].astype(F32), 0.0).astype(BF16)
    high = dot(kept, mine[half:, :], 1, 0).astype(BF16)
    rows = mine[pl.ds(last, count), :]
    for i, (one, other) in enumerate(((rows, high), (high, rows))):
        left[pl.ds(i * count, count), :] = one
        right[pl.ds(i * count, count), :] = other
    stores = []
    for s in range(width // chunk):
        at = pl.ds(s * chunk, chunk)
        held[at, :] = total[at, :] + dot(left[:, at], right[...], 0, 0)
        store = pltpu.make_async_copy(held.at[at], out.at[0, at], store_sem.at[s])
        store.start()
        stores.append(store)
    for store in stores:
        store.wait()


def in_place(array):
    return pltpu.with_memory_space_constraint(array, pltpu.HBM)


def on_device(factor_inv, sep_sizes, coupling):
    ny, nz = lax.axis_size("gy"), lax.axis_size("gz")
    width = factor_inv.shape[1]
    inter = coupling.shape[2]
    half = width // 2
    block = half // 2
    steps = width // block
    sides = 2 if nz > 2 else 1
    tail = min(TAIL, block)
    pieces = [(start, tail) for start in range(0, half, tail)]
    count = len(pieces) + 3
    extra = (-(-3 * (half // LANES) // 16) * 16, LANES)
    anywhere = pl.BlockSpec(memory_space=pl.ANY)
    inside = pl.BlockSpec(memory_space=pltpu.VMEM)
    total, mine, last = pl.pallas_call(
        functools.partial(gather_kernel, ny, nz, pieces),
        out_shape=(
            pltpu.VMEM((inter, inter), F32),
            pltpu.VMEM((width, inter), BF16),
            pltpu.VMEM((tail, half), BF16),
        ),
        in_specs=[pl.BlockSpec(memory_space=pltpu.SMEM), anywhere, anywhere],
        out_specs=(inside, inside, inside),
        scratch_shapes=[
            pltpu.VMEM((width, width), BF16),
            pltpu.VMEM((sides, width, inter), BF16),
            pltpu.VMEM((sides, width, width), BF16),
            pltpu.VMEM((inter, width), BF16),
            pltpu.VMEM((half, half), BF16),
            pltpu.VMEM(extra, BF16),
            pltpu.VMEM((half, half), BF16),
            pltpu.VMEM((half, half), BF16),
            pltpu.VMEM(extra, BF16),
            pltpu.VMEM((half, half), BF16),
            pltpu.VMEM((2, half, half), BF16),
            pltpu.SemaphoreType.DMA((3 + steps,)),
            pltpu.SemaphoreType.DMA((2,)),
            pltpu.SemaphoreType.DMA((2,)),
            pltpu.SemaphoreType.DMA((count,)),
            pltpu.SemaphoreType.DMA((count,)),
        ],
        compiler_params=pltpu.CompilerParams(
            collective_id=0, has_side_effects=True, vmem_limit_bytes=40 * 2**20
        ),
    )(sep_sizes, in_place(factor_inv), in_place(coupling))
    return pl.pallas_call(
        finish_kernel,
        out_shape=jax.ShapeDtypeStruct((1, inter, inter), F32),
        in_specs=[inside, inside, inside],
        out_specs=anywhere,
        scratch_shapes=[
            pltpu.VMEM((2 * tail, inter), BF16),
            pltpu.VMEM((2 * tail, inter), BF16),
            pltpu.VMEM((inter, inter), F32),
            pltpu.SemaphoreType.DMA((inter // TAIL,)),
        ],
        compiler_params=pltpu.CompilerParams(vmem_limit_bytes=40 * 2**20),
    )(total, mine, last)


def solution(mesh):
    return jax.shard_map(
        on_device,
        mesh=mesh,
        in_specs=(P("gx", "gy", "gz"), P("gx", "gy", "gz"), P("gx", "gy", "gz")),
        out_specs=P("gx", "gy", "gz"),
        check_vma=False,
    )
```

```python
import functools

import jax
import jax.numpy as jnp
from jax import lax
from jax.experimental import pallas as pl
from jax.experimental.pallas import tpu as pltpu
from jax.sharding import PartitionSpec as P

MESH = pl.DeviceIdType.MESH
F32, BF16 = jnp.float32, jnp.bfloat16
LANES = 128
TAIL = 128
RELAYED = 1


def dot(lhs, rhs, left, right):
    return lax.dot_general(lhs, rhs, (((left,), (right,)), ((), ())), preferred_element_type=F32)


def grid_of(rows, cols):
    return (
        lax.broadcasted_iota(jnp.int32, (rows, cols), 0),
        lax.broadcasted_iota(jnp.int32, (rows, cols), 1),
    )


def gather_kernel(
    ny, nz, pieces, relay,
    sizes, factor, coupling,
    total, mine, tail,
    own, couple, beside, solved, mixed, extra, cross, mixed_in, extra_in, cross_in, full, passed,
    load_sem, z_send, z_recv, y_send, y_recv, pass_send, pass_recv,
):
    width = own.shape[0]
    half = width // 2
    block = half // 2
    steps = width // block
    per = half // LANES
    b, c = lax.axis_index("gy"), lax.axis_index("gz")
    above, below = b < ny - 1, b > 0
    ups, downs = c < nz - 1, c > 0
    greets = [(below, {"gy": b - 1}), (ups, {"gz": c + 1}), (downs, {"gz": c - 1})]
    awaits = [above, ups, downs]
    if relay is not None:
        far, via = relay
        greets = [(b == via, {"gy": far})] + greets + [(b == far + 1, {"gy": via})]
        awaits += [b == far, b == via]

    rows_of = [pl.ds(s * block, block) for s in range(steps)]
    factors = [pltpu.make_async_copy(factor.at[0, at], own.at[at], load_sem.at[3 + s]) for s, at in enumerate(rows_of)]
    for load in factors:
        load.start()

    barrier = pltpu.get_barrier_semaphore()
    for there, peer in greets:
        @pl.when(there)
        def _():
            pl.semaphore_signal(barrier, inc=1, device_id=peer, device_id_type=MESH)

    if nz == 2:
        z_loads = [pltpu.make_async_copy(coupling.at[1 - c], couple.at[0], load_sem.at[0])]
    else:
        z_loads = [pltpu.make_async_copy(coupling.at[e], couple.at[e], load_sem.at[e]) for e in range(2)]
    loads = z_loads + [pltpu.make_async_copy(coupling.at[2], mine, load_sem.at[2])]

    size = sizes[0, 0, 0]
    column = (lax.broadcasted_iota(jnp.int32, (1, width), 1) < size).astype(F32).astype(BF16)
    for s in range(steps):
        rows = rows_of[s]
        row = (lax.broadcasted_iota(jnp.int32, (block, 1), 0) + s * block < size).astype(F32).astype(BF16)
        factors[s].wait()
        own[rows, :] = own[rows, :] * row * column

    for load in loads:
        load.start()

    z_copies = []
    for k, (goes, to, comes) in enumerate(((ups, c + 1, downs), (downs, c - 1, ups))):
        copy = pltpu.make_async_remote_copy(
            src_ref=own, dst_ref=beside.at[k if nz > 2 else 0], send_sem=z_send.at[k], recv_sem=z_recv.at[k],
            device_id={"gz": to}, device_id_type=MESH,
        )
        z_copies.append((goes, comes, copy))

    def y_copy(src, dst, k):
        return pltpu.make_async_remote_copy(
            src_ref=src, dst_ref=dst, send_sem=y_send.at[k], recv_sem=y_recv.at[k],
            device_id={"gy": b + 1}, device_id_type=MESH,
        )

    tops = [pl.ds(s * block, block) for s in range(2)]
    mixes = [y_copy(mixed.at[at], mixed_in.at[at], s) for s, at in enumerate(tops)]
    mixes.append(y_copy(extra, extra_in, 2))
    crosses = []
    for k, (start, count) in enumerate(pieces):
        rows = pl.ds(start, count)
        dst = cross_in.at[rows] if k < len(pieces) - 1 else tail
        crosses.append(y_copy(cross.at[rows], dst, k + 3))

    first_hop = second_hop = None
    if relay is not None:
        start, count = pieces[RELAYED]
        first_hop = pltpu.make_async_remote_copy(
            src_ref=cross.at[pl.ds(start, count)], dst_ref=passed,
            send_sem=y_send.at[RELAYED + 3], recv_sem=pass_recv.at[0],
            device_id={"gy": via}, device_id_type=MESH,
        )
        second_hop = pltpu.make_async_remote_copy(
            src_ref=passed, dst_ref=cross_in.at[pl.ds(start, count)],
            send_sem=pass_send.at[0], recv_sem=y_recv.at[RELAYED + 3],
            device_id={"gy": far + 1}, device_id_type=MESH,
        )

    def send_cross(k):
        if relay is None or k != RELAYED:
            crosses[k].start()
        else:
            @pl.when(b == far)
            def _():
                first_hop.start()

            @pl.when(b != far)
            def _():
                crosses[k].start()

    def make_cross(k):
        start, count = pieces[k]
        cross[pl.ds(start, count), :] = dot(own[:, pl.ds(start, count)], own[:, half:], 0, 0).astype(BF16)

    @pl.when(above)
    def _():
        make_cross(0)

    pl.semaphore_wait(barrier, sum(there.astype(jnp.int32) for there in awaits))

    @pl.when(above)
    def _():
        crosses[0].start()

    for goes, comes, copy in z_copies:
        @pl.when(goes)
        def _():
            copy.start()

    @pl.when(above)
    def _():
        r, q = grid_of(block, block)
        lines = []
        first = dot(own[:, :block], own[:, :half], 0, 0)
        second = dot(own[:, half : half + block], own[:, half : half + block], 0, 0)
        mixed[:block, :block] = jnp.where(r <= q, first[:, :block], second).astype(BF16)
        mixed[:block, block:] = first[:, block:].astype(BF16)
        mixes[0].start()
        lines.append((first[:, :block], second))
        second = dot(own[:, half + block :], own[:, half:], 0, 0)
        first = dot(own[:, block:half], own[:, block:half], 0, 0)
        mixed[block:, :block] = second[:, :block].astype(BF16)
        mixed[block:, block:] = jnp.where(r <= q, first, second[:, block:]).astype(BF16)
        mixes[1].start()
        lines.append((first, second[:, block:]))
        at = lax.broadcasted_iota(jnp.int32, extra.shape, 0)
        filled = jnp.zeros(extra.shape, F32)
        for s, pair in enumerate(lines):
            one, two = (jnp.sum(jnp.where(r == q, value, 0.0), axis=0, keepdims=True) for value in pair)
            high = two.astype(BF16).astype(F32)
            for group, line in enumerate((high, one - one.astype(BF16).astype(F32), two - high)):
                for i in range(block // LANES):
                    place = group * per + s * (block // LANES) + i
                    filled = jnp.where(at == place, line[:, i * LANES : (i + 1) * LANES], filled)
        extra[...] = filled.astype(BF16)
        mixes[2].start()
        for k in range(1, len(pieces)):
            make_cross(k)
            send_cross(k)

    if relay is not None:
        @pl.when(b == via)
        def _():
            first_hop.wait_recv()
            second_hop.start()

    for load in loads:
        load.wait()

    def z_slot(slot, k, fresh):
        solved[...] = dot(beside[k], couple[slot], 1, 0).astype(BF16)
        term = dot(solved[...], solved[...], 0, 0)
        total[...] = term if fresh else total[...] + term

    if nz == 2:
        for goes, comes, copy in z_copies:
            @pl.when(comes)
            def _():
                copy.wait_recv()
        z_slot(0, 0, True)
    else:
        total[...] = jnp.zeros_like(total)
        for k, (goes, comes, copy) in enumerate(z_copies):
            @pl.when(comes)
            def _():
                copy.wait_recv()
                z_slot(k, k, False)


    @pl.when(below)
    def _():
        def use_cross(k):
            start, count = pieces[k]
            crosses[k].wait_recv()
            high = dot(cross_in[pl.ds(start, count), :], mine[half:, :], 1, 0).astype(BF16)
            own_rows = mine[pl.ds(start, count), :]
            for i, value in enumerate((own_rows, high, own_rows)):
                solved[pl.ds(i * count, count), :] = value

            total[...] = total[...] + dot(solved[pl.ds(0, 2 * count), :], solved[pl.ds(count, 2 * count), :], 0, 0)

        use_cross(0)
        for copy in mixes:
            copy.wait_recv()
        r, q = grid_of(half, half)
        value = mixed_in[...].astype(F32)
        turned = value.T
        extras = extra_in[...].astype(F32)

        def line(group):
            return jnp.concatenate([extras[group * per + i : group * per + i + 1, :] for i in range(per)], axis=1)

        full[0] = jnp.where(r <= q, value, turned).astype(BF16)
        full[1] = jnp.where(r > q, value, jnp.where(r == q, line(0), turned)).astype(BF16)
        for i in range(2):
            low = jnp.sum(jnp.where(r == q, line(1 + i), 0.0), axis=1, keepdims=True)
            rows = pl.ds(i * half, half)
            piece = mine[rows, :]
            solved[rows, :] = (dot(full[i], piece, 1, 0) + low * piece.astype(F32)).astype(BF16)

        total[...] = total[...] + dot(mine[...], solved[...], 0, 0)

        for k in range(1, len(pieces) - 1):
            use_cross(k)
        crosses[-1].wait_recv()

    for goes, comes, copy in z_copies:
        @pl.when(goes)
        def _():
            copy.wait_send()

    @pl.when(above)
    def _():
        for copy in mixes + crosses:
            copy.wait_send()

    if relay is not None:
        @pl.when(b == via)
        def _():
            second_hop.wait_send()


def finish_kernel(total, mine, tail, out, left, right, held, store_sem):
    count, half = tail.shape
    width = total.shape[0]
    last = tail.shape[1] - count
    chunk = TAIL

    kept = jnp.where(lax.axis_index("gy") > 0, tail[...].astype(F32), 0.0).astype(BF16)
    high = dot(kept, mine[half:, :], 1, 0).astype(BF16)
    rows = mine[pl.ds(last, count), :]
    for i, (one, other) in enumerate(((rows, high), (high, rows))):
        left[pl.ds(i * count, count), :] = one
        right[pl.ds(i * count, count), :] = other
    stores = []
    for s in range(width // chunk):
        at = pl.ds(s * chunk, chunk)
        held[at, :] = total[at, :] + dot(left[:, at], right[...], 0, 0)
        store = pltpu.make_async_copy(held.at[at], out.at[0, at], store_sem.at[s])
        store.start()
        stores.append(store)
    for store in stores:
        store.wait()


def in_place(array):
    return pltpu.with_memory_space_constraint(array, pltpu.HBM)


def on_device(relay, factor_inv, sep_sizes, coupling):
    ny, nz = lax.axis_size("gy"), lax.axis_size("gz")
    width = factor_inv.shape[1]
    inter = coupling.shape[2]
    half = width // 2
    block = half // 2
    steps = width // block
    sides = 2 if nz > 2 else 1
    tail = min(TAIL, block)
    pieces = [(start, tail) for start in range(0, half, tail)]
    count = len(pieces) + 3
    extra = (-(-3 * (half // LANES) // 16) * 16, LANES)
    anywhere = pl.BlockSpec(memory_space=pl.ANY)
    inside = pl.BlockSpec(memory_space=pltpu.VMEM)
    total, mine, last = pl.pallas_call(
        functools.partial(gather_kernel, ny, nz, pieces, relay),
        out_shape=(
            pltpu.VMEM((inter, inter), F32),
            pltpu.VMEM((width, inter), BF16),
            pltpu.VMEM((tail, half), BF16),
        ),
        in_specs=[pl.BlockSpec(memory_space=pltpu.SMEM), anywhere, anywhere],
        out_specs=(inside, inside, inside),
        scratch_shapes=[
            pltpu.VMEM((width, width), BF16),
            pltpu.VMEM((sides, width, inter), BF16),
            pltpu.VMEM((sides, width, width), BF16),
            pltpu.VMEM((width, inter), BF16),
            pltpu.VMEM((half, half), BF16),
            pltpu.VMEM(extra, BF16),
            pltpu.VMEM((half, half), BF16),
            pltpu.VMEM((half, half), BF16),
            pltpu.VMEM(extra, BF16),
            pltpu.VMEM((half, half), BF16),
            pltpu.VMEM((2, half, half), BF16),
            pltpu.VMEM((pieces[RELAYED][1], half), BF16),
            pltpu.SemaphoreType.DMA((3 + steps,)),
            pltpu.SemaphoreType.DMA((2,)),
            pltpu.SemaphoreType.DMA((2,)),
            pltpu.SemaphoreType.DMA((count,)),
            pltpu.SemaphoreType.DMA((count,)),
            pltpu.SemaphoreType.DMA((1,)),
            pltpu.SemaphoreType.DMA((1,)),
        ],
        compiler_params=pltpu.CompilerParams(
            collective_id=0, has_side_effects=True, vmem_limit_bytes=40 * 2**20
        ),
    )(sep_sizes, in_place(factor_inv), in_place(coupling))
    return pl.pallas_call(
        finish_kernel,
        out_shape=jax.ShapeDtypeStruct((1, inter, inter), F32),
        in_specs=[inside, inside, inside],
        out_specs=anywhere,
        scratch_shapes=[
            pltpu.VMEM((2 * tail, inter), BF16),
            pltpu.VMEM((2 * tail, inter), BF16),
            pltpu.VMEM((inter, inter), F32),
            pltpu.SemaphoreType.DMA((inter // TAIL,)),
        ],
        compiler_params=pltpu.CompilerParams(vmem_limit_bytes=40 * 2**20),
    )(total, mine, last)


def relay_of(mesh):
    line = [getattr(mesh.devices[0, b, 0], "coords", None) for b in range(mesh.shape["gy"])]
    if any(at is None for at in line):
        return None
    for b in range(len(line) - 1):
        here, there = line[b], line[b + 1]
        apart = [i for i in range(len(here)) if here[i] != there[i]]
        if len(apart) == 2 and all(abs(here[i] - there[i]) == 1 for i in apart):
            corner = list(here)
            corner[apart[1]] = there[apart[1]]
            if list(corner) in [list(at) for at in line]:
                return b, [list(at) for at in line].index(list(corner))
    return None


def solution(mesh):
    return jax.shard_map(
        functools.partial(on_device, relay_of(mesh)),
        mesh=mesh,
        in_specs=(P("gx", "gy", "gz"), P("gx", "gy", "gz"), P("gx", "gy", "gz")),
        out_specs=P("gx", "gy", "gz"),
        check_vma=False,
    )
```

```python
import functools

import jax
import jax.numpy as jnp
from jax import lax
from jax.experimental import pallas as pl
from jax.experimental.pallas import tpu as pltpu
from jax.sharding import PartitionSpec as P

MESH = pl.DeviceIdType.MESH
F32, BF16 = jnp.float32, jnp.bfloat16
LANES = 128
TAIL = 128
TIP = 128
LATE = 32
RELAYED = 1


def dot(lhs, rhs, left, right):
    return lax.dot_general(lhs, rhs, (((left,), (right,)), ((), ())), preferred_element_type=F32)


def grid_of(rows, cols):
    return (
        lax.broadcasted_iota(jnp.int32, (rows, cols), 0),
        lax.broadcasted_iota(jnp.int32, (rows, cols), 1),
    )


def gather_kernel(
    ny, nz, pieces, relay,
    sizes, factor, coupling,
    total, mine, tail, ready,
    own, couple, beside, solved, mixed, extra, cross, mixed_in, extra_in, cross_in, full, passed,
    load_sem, z_send, z_recv, y_send, y_recv, pass_send, pass_recv,
):
    width = own.shape[0]
    half = width // 2
    block = half // 2
    steps = width // block
    per = half // LANES
    b, c = lax.axis_index("gy"), lax.axis_index("gz")
    above, below = b < ny - 1, b > 0
    ups, downs = c < nz - 1, c > 0
    greets = [(below, {"gy": b - 1}), (ups, {"gz": c + 1}), (downs, {"gz": c - 1})]
    awaits = [above, ups, downs]
    if relay is not None:
        far, via = relay
        greets = [(b == via, {"gy": far})] + greets + [(b == far + 1, {"gy": via})]
        awaits += [b == far, b == via]

    barrier = pltpu.get_barrier_semaphore()
    for there, peer in greets:
        @pl.when(there)
        def _():
            pl.semaphore_signal(barrier, inc=1, device_id=peer, device_id_type=MESH)

    spans = ((0, TIP), (half, half + TIP), (TIP, half), (half + TIP, width))
    parts = [pl.ds(start, end - start) for start, end in spans]
    factors = [pltpu.make_async_copy(factor.at[0, :, at], own.at[:, at], load_sem.at[3 + s]) for s, at in enumerate(parts)]
    for load in factors:
        load.start()

    if nz == 2:
        z_loads = [pltpu.make_async_copy(coupling.at[1 - c], couple.at[0], load_sem.at[0])]
    else:
        z_loads = [pltpu.make_async_copy(coupling.at[e], couple.at[e], load_sem.at[e]) for e in range(2)]
    loads = z_loads + [pltpu.make_async_copy(coupling.at[2], mine, load_sem.at[2])]

    size = sizes[0, 0, 0]
    row = (lax.broadcasted_iota(jnp.int32, (width, 1), 0) < size).astype(F32).astype(BF16)

    def mask(s):
        start, end = spans[s]
        column = (lax.broadcasted_iota(jnp.int32, (1, end - start), 1) + start < size).astype(F32).astype(BF16)
        factors[s].wait()
        own[:, parts[s]] = own[:, parts[s]] * row * column

    mask(0)
    mask(1)

    @pl.when(above)
    def _():
        tip = dot(own[:, :TIP], own[:, half : half + TIP], 0, 0)
        cross[:TIP, :TIP] = tip.astype(BF16)


    z_copies = []
    for k, (goes, to, comes) in enumerate(((ups, c + 1, downs), (downs, c - 1, ups))):
        copy = pltpu.make_async_remote_copy(
            src_ref=own, dst_ref=beside.at[k if nz > 2 else 0], send_sem=z_send.at[k], recv_sem=z_recv.at[k],
            device_id={"gz": to}, device_id_type=MESH,
        )
        z_copies.append((goes, comes, copy))

    def y_copy(src, dst, k):
        return pltpu.make_async_remote_copy(
            src_ref=src, dst_ref=dst, send_sem=y_send.at[k], recv_sem=y_recv.at[k],
            device_id={"gy": b + 1}, device_id_type=MESH,
        )

    tops = [pl.ds(s * block, block) for s in range(2)]
    mixes = [y_copy(mixed.at[at], mixed_in.at[at], s) for s, at in enumerate(tops)]
    mixes.append(y_copy(extra, extra_in, 2))
    crosses = []
    for k, (start, count) in enumerate(pieces):
        rows = pl.ds(start, count)
        dst = cross_in.at[rows] if k < len(pieces) - 1 else tail
        if k == 0:
            crosses.append(y_copy(cross.at[rows, pl.ds(TIP, half - TIP)], cross_in.at[rows, pl.ds(TIP, half - TIP)], 3))
        else:
            crosses.append(y_copy(cross.at[rows], dst, k + 3))
    crosses.append(y_copy(cross.at[pl.ds(0, TIP), pl.ds(0, TIP)], cross_in.at[pl.ds(0, TIP), pl.ds(0, TIP)], len(pieces) + 3))

    first_hop = second_hop = None
    if relay is not None:
        start, count = pieces[RELAYED]
        first_hop = pltpu.make_async_remote_copy(
            src_ref=cross.at[pl.ds(start, count)], dst_ref=passed,
            send_sem=y_send.at[RELAYED + 3], recv_sem=pass_recv.at[0],
            device_id={"gy": via}, device_id_type=MESH,
        )
        second_hop = pltpu.make_async_remote_copy(
            src_ref=passed, dst_ref=cross_in.at[pl.ds(start, count)],
            send_sem=pass_send.at[0], recv_sem=y_recv.at[RELAYED + 3],
            device_id={"gy": far + 1}, device_id_type=MESH,
        )

    def send_cross(k):
        if relay is None or k != RELAYED:
            crosses[k].start()
        else:
            @pl.when(b == far)
            def _():
                first_hop.start()

            @pl.when(b != far)
            def _():
                crosses[k].start()

    def make_cross(k):
        start, count = pieces[k]
        cross[pl.ds(start, count), :] = dot(own[:, pl.ds(start, count)], own[:, half:], 0, 0).astype(BF16)

    pl.semaphore_wait(barrier, sum(there.astype(jnp.int32) for there in awaits))

    @pl.when(above)
    def _():
        crosses[-1].start()

    mask(2)
    mask(3)
    for load in loads:
        load.start()

    @pl.when(above)
    def _():
        edge = dot(own[:, :TIP], own[:, half + TIP :], 0, 0)
        cross[:TIP, TIP:] = edge.astype(BF16)
        crosses[0].start()

    for goes, comes, copy in z_copies:
        @pl.when(goes)
        def _():
            copy.start()

    @pl.when(above)
    def _():
        r, q = grid_of(block, block)
        lines = []
        first = dot(own[:, :block], own[:, :half], 0, 0)
        second = dot(own[:, half : half + block], own[:, half : half + block], 0, 0)
        mixed[:block, :block] = jnp.where(r <= q, first[:, :block], second).astype(BF16)
        mixed[:block, block:] = first[:, block:].astype(BF16)
        mixes[0].start()
        lines.append((first[:, :block], second))
        second = dot(own[:, half + block :], own[:, half:], 0, 0)
        first = dot(own[:, block:half], own[:, block:half], 0, 0)
        mixed[block:, :block] = second[:, :block].astype(BF16)
        mixed[block:, block:] = jnp.where(r <= q, first, second[:, block:]).astype(BF16)
        mixes[1].start()
        lines.append((first, second[:, block:]))
        at = lax.broadcasted_iota(jnp.int32, extra.shape, 0)
        filled = jnp.zeros(extra.shape, F32)
        for s, pair in enumerate(lines):
            one, two = (jnp.sum(jnp.where(r == q, value, 0.0), axis=0, keepdims=True) for value in pair)
            high = two.astype(BF16).astype(F32)
            for group, line in enumerate((high, one - one.astype(BF16).astype(F32), two - high)):
                for i in range(block // LANES):
                    place = group * per + s * (block // LANES) + i
                    filled = jnp.where(at == place, line[:, i * LANES : (i + 1) * LANES], filled)
        extra[...] = filled.astype(BF16)
        mixes[2].start()
        for k in range(1, len(pieces)):
            make_cross(k)
            send_cross(k)

    if relay is not None:
        @pl.when(b == via)
        def _():
            first_hop.wait_recv()
            second_hop.start()

    for load in loads:
        load.wait()

    def z_slot(slot, k, fresh):
        solved[...] = dot(beside[k], couple[slot], 1, 0).astype(BF16)
        term = dot(solved[...], solved[...], 0, 0)
        total[...] = term if fresh else total[...] + term

    if nz == 2:
        for goes, comes, copy in z_copies:
            @pl.when(comes)
            def _():
                copy.wait_recv()
        z_slot(0, 0, True)
    else:
        total[...] = jnp.zeros_like(total)
        for k, (goes, comes, copy) in enumerate(z_copies):
            @pl.when(comes)
            def _():
                copy.wait_recv()
                z_slot(k, k, False)


    @pl.when(below)
    def _():
        def use_cross(k):
            start, count = pieces[k]
            crosses[k].wait_recv()
            if k == 0:
                crosses[-1].wait_recv()
            high = dot(cross_in[pl.ds(start, count), :], mine[half:, :], 1, 0).astype(BF16)
            own_rows = mine[pl.ds(start, count), :]
            for i, value in enumerate((own_rows, high, own_rows)):
                solved[pl.ds(i * count, count), :] = value

            total[...] = total[...] + dot(solved[pl.ds(0, 2 * count), :], solved[pl.ds(count, 2 * count), :], 0, 0)

        use_cross(0)
        for copy in mixes:
            copy.wait_recv()
        r, q = grid_of(half, half)
        value = mixed_in[...].astype(F32)
        turned = value.T
        extras = extra_in[...].astype(F32)

        def line(group):
            return jnp.concatenate([extras[group * per + i : group * per + i + 1, :] for i in range(per)], axis=1)

        full[0] = jnp.where(r <= q, value, turned).astype(BF16)
        full[1] = jnp.where(r > q, value, jnp.where(r == q, line(0), turned)).astype(BF16)
        for i in range(2):
            low = jnp.sum(jnp.where(r == q, line(1 + i), 0.0), axis=1, keepdims=True)
            rows = pl.ds(i * half, half)
            piece = mine[rows, :]
            solved[rows, :] = (dot(full[i], piece, 1, 0) + low * piece.astype(F32)).astype(BF16)

        total[...] = total[...] + dot(mine[...], solved[...], 0, 0)

        for k in range(1, len(pieces) - 2):
            use_cross(k)
        start, count = pieces[-2]
        crosses[-3].wait_recv()
        ready[...] = dot(cross_in[pl.ds(start, count), :], mine[half:, :], 1, 0).astype(BF16)
        crosses[-2].wait_recv()

    @pl.when(jnp.logical_not(below))
    def _():
        ready[...] = jnp.zeros_like(ready)

    for goes, comes, copy in z_copies:
        @pl.when(goes)
        def _():
            copy.wait_send()

    @pl.when(above)
    def _():
        for copy in mixes + crosses:
            copy.wait_send()

    if relay is not None:
        @pl.when(b == via)
        def _():
            second_hop.wait_send()


def finish_kernel(total, mine, tail, ready, out, left, right, held, store_sem):
    late, half = tail.shape
    early = ready.shape[0]
    count = early + late
    width = total.shape[0]
    chunk = TAIL

    kept = jnp.where(lax.axis_index("gy") > 0, tail[...].astype(F32), 0.0).astype(BF16)
    rows = mine[pl.ds(half - count, count), :]
    left[:count, :] = rows
    right[count:, :] = rows
    left[count : count + early, :] = ready[...]
    right[:early, :] = ready[...]
    high = dot(kept, mine[half:, :], 1, 0).astype(BF16)
    left[count + early :, :] = high
    right[early:count, :] = high
    stores = []
    for s in range(width // chunk):
        at = pl.ds(s * chunk, chunk)
        held[at, :] = total[at, :] + dot(left[:, at], right[...], 0, 0)
        store = pltpu.make_async_copy(held.at[at], out.at[0, at], store_sem.at[s])
        store.start()
        stores.append(store)
    for store in stores:
        store.wait()


def in_place(array):
    return pltpu.with_memory_space_constraint(array, pltpu.HBM)


def on_device(relay, factor_inv, sep_sizes, coupling):
    ny, nz = lax.axis_size("gy"), lax.axis_size("gz")
    width = factor_inv.shape[1]
    inter = coupling.shape[2]
    half = width // 2
    block = half // 2
    steps = width // block
    sides = 2 if nz > 2 else 1
    tail = min(TAIL, block)
    pieces = [(start, tail) for start in range(0, half, tail)]
    early = tail - LATE
    pieces = pieces[:-1] + [(half - tail, early), (half - LATE, LATE)]
    count = len(pieces) + 4
    extra = (-(-3 * (half // LANES) // 16) * 16, LANES)
    anywhere = pl.BlockSpec(memory_space=pl.ANY)
    inside = pl.BlockSpec(memory_space=pltpu.VMEM)
    total, mine, last, ready = pl.pallas_call(
        functools.partial(gather_kernel, ny, nz, pieces, relay),
        out_shape=(
            pltpu.VMEM((inter, inter), F32),
            pltpu.VMEM((width, inter), BF16),
            pltpu.VMEM((LATE, half), BF16),
            pltpu.VMEM((early, inter), BF16),
        ),
        in_specs=[pl.BlockSpec(memory_space=pltpu.SMEM), anywhere, anywhere],
        out_specs=(inside,) * 4,
        scratch_shapes=[
            pltpu.VMEM((width, width), BF16),
            pltpu.VMEM((sides, width, inter), BF16),
            pltpu.VMEM((sides, width, width), BF16),
            pltpu.VMEM((width, inter), BF16),
            pltpu.VMEM((half, half), BF16),
            pltpu.VMEM(extra, BF16),
            pltpu.VMEM((half, half), BF16),
            pltpu.VMEM((half, half), BF16),
            pltpu.VMEM(extra, BF16),
            pltpu.VMEM((half, half), BF16),
            pltpu.VMEM((2, half, half), BF16),
            pltpu.VMEM((pieces[RELAYED][1], half), BF16),
            pltpu.SemaphoreType.DMA((7,)),
            pltpu.SemaphoreType.DMA((2,)),
            pltpu.SemaphoreType.DMA((2,)),
            pltpu.SemaphoreType.DMA((count,)),
            pltpu.SemaphoreType.DMA((count,)),
            pltpu.SemaphoreType.DMA((1,)),
            pltpu.SemaphoreType.DMA((1,)),
        ],
        compiler_params=pltpu.CompilerParams(
            collective_id=0, has_side_effects=True, vmem_limit_bytes=40 * 2**20
        ),
    )(sep_sizes, in_place(factor_inv), in_place(coupling))
    return pl.pallas_call(
        finish_kernel,
        out_shape=jax.ShapeDtypeStruct((1, inter, inter), F32),
        in_specs=[inside] * 4,
        out_specs=anywhere,
        scratch_shapes=[
            pltpu.VMEM((2 * tail, inter), BF16),
            pltpu.VMEM((2 * tail, inter), BF16),
            pltpu.VMEM((inter, inter), F32),
            pltpu.SemaphoreType.DMA((inter // TAIL,)),
        ],
        compiler_params=pltpu.CompilerParams(vmem_limit_bytes=40 * 2**20),
    )(total, mine, last, ready)


def relay_of(mesh):
    line = [getattr(mesh.devices[0, b, 0], "coords", None) for b in range(mesh.shape["gy"])]
    if any(at is None for at in line):
        return None
    for b in range(len(line) - 1):
        here, there = line[b], line[b + 1]
        apart = [i for i in range(len(here)) if here[i] != there[i]]
        if len(apart) == 2 and all(abs(here[i] - there[i]) == 1 for i in apart):
            corner = list(here)
            corner[apart[1]] = there[apart[1]]
            if list(corner) in [list(at) for at in line]:
                return b, [list(at) for at in line].index(list(corner))
    return None


def solution(mesh):
    return jax.shard_map(
        functools.partial(on_device, relay_of(mesh)),
        mesh=mesh,
        in_specs=(P("gx", "gy", "gz"), P("gx", "gy", "gz"), P("gx", "gy", "gz")),
        out_specs=P("gx", "gy", "gz"),
        check_vma=False,
    )
```

```python
import functools

import jax
import jax.numpy as jnp
from jax import lax
from jax.experimental import pallas as pl
from jax.experimental.pallas import tpu as pltpu
from jax.sharding import PartitionSpec as P

MESH = pl.DeviceIdType.MESH
F32, BF16 = jnp.float32, jnp.bfloat16
LANES = 128
TAIL = 128
TIP = 128
LATE = 32
RELAYED = 1


def dot(lhs, rhs, left, right):
    return lax.dot_general(lhs, rhs, (((left,), (right,)), ((), ())), preferred_element_type=F32)


def grid_of(rows, cols):
    return (
        lax.broadcasted_iota(jnp.int32, (rows, cols), 0),
        lax.broadcasted_iota(jnp.int32, (rows, cols), 1),
    )


def gather_kernel(
    ny, nz, pieces, relay,
    sizes, factor, coupling,
    total, mine, tail, ready,
    own, couple, beside, solved, mixed, extra, cross, mixed_in, extra_in, cross_in, full, passed,
    load_sem, z_send, z_recv, y_send, y_recv, pass_send, pass_recv,
):
    width = own.shape[0]
    half = width // 2
    block = half // 2
    steps = width // block
    per = half // LANES
    b, c = lax.axis_index("gy"), lax.axis_index("gz")
    above, below = b < ny - 1, b > 0
    ups, downs = c < nz - 1, c > 0
    greets = [(below, {"gy": b - 1}), (ups, {"gz": c + 1}), (downs, {"gz": c - 1})]
    awaits = [above, ups, downs]
    if relay is not None:
        far, via = relay
        greets += [(b == via, {"gy": far}), (b == far + 1, {"gy": via})]
        awaits += [b == far, b == via]

    barrier = pltpu.get_barrier_semaphore()
    for there, peer in greets:
        @pl.when(there)
        def _():
            pl.semaphore_signal(barrier, inc=1, device_id=peer, device_id_type=MESH)

    spans = ((0, TIP), (half, half + TIP), (TIP, half), (half + TIP, width))
    parts = [pl.ds(start, end - start) for start, end in spans]
    factors = [pltpu.make_async_copy(factor.at[0, :, at], own.at[:, at], load_sem.at[3 + s]) for s, at in enumerate(parts)]
    for load in factors:
        load.start()

    if nz == 2:
        z_loads = [pltpu.make_async_copy(coupling.at[1 - c], couple.at[0], load_sem.at[0])]
    else:
        z_loads = [pltpu.make_async_copy(coupling.at[e], couple.at[e], load_sem.at[e]) for e in range(2)]
    loads = z_loads + [pltpu.make_async_copy(coupling.at[2], mine, load_sem.at[2])]

    size = sizes[0, 0, 0]
    row = (lax.broadcasted_iota(jnp.int32, (width, 1), 0) < size).astype(F32).astype(BF16)

    def mask(s):
        start, end = spans[s]
        column = (lax.broadcasted_iota(jnp.int32, (1, end - start), 1) + start < size).astype(F32).astype(BF16)
        factors[s].wait()
        own[:, parts[s]] = own[:, parts[s]] * row * column

    mask(0)
    mask(1)

    @pl.when(above)
    def _():
        tip = dot(own[:, :TIP], own[:, half : half + TIP], 0, 0)
        cross[:TIP, :TIP] = tip.astype(BF16)


    z_copies = []
    for k, (goes, to, comes) in enumerate(((ups, c + 1, downs), (downs, c - 1, ups))):
        copy = pltpu.make_async_remote_copy(
            src_ref=own, dst_ref=beside.at[k if nz > 2 else 0], send_sem=z_send.at[k], recv_sem=z_recv.at[k],
            device_id={"gz": to}, device_id_type=MESH,
        )
        z_copies.append((goes, comes, copy))

    def y_copy(src, dst, k):
        return pltpu.make_async_remote_copy(
            src_ref=src, dst_ref=dst, send_sem=y_send.at[k], recv_sem=y_recv.at[k],
            device_id={"gy": b + 1}, device_id_type=MESH,
        )

    tops = [pl.ds(s * block, block) for s in range(2)]
    mixes = [y_copy(mixed.at[at], mixed_in.at[at], s) for s, at in enumerate(tops)]
    mixes.append(y_copy(extra, extra_in, 2))
    crosses = []
    for k, (start, count) in enumerate(pieces):
        rows = pl.ds(start, count)
        dst = cross_in.at[rows] if k < len(pieces) - 1 else tail
        if k == 0:
            crosses.append(y_copy(cross.at[rows, pl.ds(TIP, half - TIP)], cross_in.at[rows, pl.ds(TIP, half - TIP)], 3))
        else:
            crosses.append(y_copy(cross.at[rows], dst, k + 3))
    crosses.append(y_copy(cross.at[pl.ds(0, TIP), pl.ds(0, TIP)], cross_in.at[pl.ds(0, TIP), pl.ds(0, TIP)], len(pieces) + 3))

    first_hop = second_hop = None
    if relay is not None:
        start, count = pieces[RELAYED]
        first_hop = pltpu.make_async_remote_copy(
            src_ref=cross.at[pl.ds(start, count)], dst_ref=passed,
            send_sem=y_send.at[RELAYED + 3], recv_sem=pass_recv.at[0],
            device_id={"gy": via}, device_id_type=MESH,
        )
        second_hop = pltpu.make_async_remote_copy(
            src_ref=passed, dst_ref=cross_in.at[pl.ds(start, count)],
            send_sem=pass_send.at[0], recv_sem=y_recv.at[RELAYED + 3],
            device_id={"gy": far + 1}, device_id_type=MESH,
        )

    def send_cross(k):
        if relay is None or k != RELAYED:
            crosses[k].start()
        else:
            @pl.when(b == far)
            def _():
                first_hop.start()

            @pl.when(b != far)
            def _():
                crosses[k].start()

    def make_cross(k):
        start, count = pieces[k]
        cross[pl.ds(start, count), :] = dot(own[:, pl.ds(start, count)], own[:, half:], 0, 0).astype(BF16)

    mask(2)
    mask(3)
    for load in loads:
        load.start()

    pl.semaphore_wait(barrier, sum(there.astype(jnp.int32) for there in awaits))

    @pl.when(above)
    def _():
        crosses[-1].start()

    @pl.when(above)
    def _():
        edge = dot(own[:, :TIP], own[:, half + TIP :], 0, 0)
        cross[:TIP, TIP:] = edge.astype(BF16)
        crosses[0].start()

    for goes, comes, copy in z_copies:
        @pl.when(goes)
        def _():
            copy.start()

    @pl.when(above)
    def _():
        r, q = grid_of(block, block)
        lines = []
        first = dot(own[:, :block], own[:, :half], 0, 0)
        second = dot(own[:, half : half + block], own[:, half : half + block], 0, 0)
        mixed[:block, :block] = jnp.where(r <= q, first[:, :block], second).astype(BF16)
        mixed[:block, block:] = first[:, block:].astype(BF16)
        mixes[0].start()
        lines.append((first[:, :block], second))
        second = dot(own[:, half + block :], own[:, half:], 0, 0)
        first = dot(own[:, block:half], own[:, block:half], 0, 0)
        mixed[block:, :block] = second[:, :block].astype(BF16)
        mixed[block:, block:] = jnp.where(r <= q, first, second[:, block:]).astype(BF16)
        mixes[1].start()
        lines.append((first, second[:, block:]))
        at = lax.broadcasted_iota(jnp.int32, extra.shape, 0)
        filled = jnp.zeros(extra.shape, F32)
        for s, pair in enumerate(lines):
            one, two = (jnp.sum(jnp.where(r == q, value, 0.0), axis=0, keepdims=True) for value in pair)
            high = two.astype(BF16).astype(F32)
            for group, line in enumerate((high, one - one.astype(BF16).astype(F32), two - high)):
                for i in range(block // LANES):
                    place = group * per + s * (block // LANES) + i
                    filled = jnp.where(at == place, line[:, i * LANES : (i + 1) * LANES], filled)
        extra[...] = filled.astype(BF16)
        mixes[2].start()
        for k in range(1, len(pieces)):
            make_cross(k)
            send_cross(k)

    if relay is not None:
        @pl.when(b == via)
        def _():
            first_hop.wait_recv()
            second_hop.start()

    for load in loads:
        load.wait()

    def z_slot(slot, k, fresh):
        solved[...] = dot(beside[k], couple[slot], 1, 0).astype(BF16)
        term = dot(solved[...], solved[...], 0, 0)
        total[...] = term if fresh else total[...] + term

    if nz == 2:
        for goes, comes, copy in z_copies:
            @pl.when(comes)
            def _():
                copy.wait_recv()
        z_slot(0, 0, True)
    else:
        total[...] = jnp.zeros_like(total)
        for k, (goes, comes, copy) in enumerate(z_copies):
            @pl.when(comes)
            def _():
                copy.wait_recv()
                z_slot(k, k, False)


    @pl.when(below)
    def _():
        def use_cross(k):
            start, count = pieces[k]
            crosses[k].wait_recv()
            if k == 0:
                crosses[-1].wait_recv()
            high = dot(cross_in[pl.ds(start, count), :], mine[half:, :], 1, 0).astype(BF16)
            own_rows = mine[pl.ds(start, count), :]
            for i, value in enumerate((own_rows, high, own_rows)):
                solved[pl.ds(i * count, count), :] = value

            total[...] = total[...] + dot(solved[pl.ds(0, 2 * count), :], solved[pl.ds(count, 2 * count), :], 0, 0)

        use_cross(0)
        for copy in mixes:
            copy.wait_recv()
        r, q = grid_of(half, half)
        value = mixed_in[...].astype(F32)
        turned = value.T
        extras = extra_in[...].astype(F32)

        def line(group):
            return jnp.concatenate([extras[group * per + i : group * per + i + 1, :] for i in range(per)], axis=1)

        full[0] = jnp.where(r <= q, value, turned).astype(BF16)
        full[1] = jnp.where(r > q, value, jnp.where(r == q, line(0), turned)).astype(BF16)
        for i in range(2):
            low = jnp.sum(jnp.where(r == q, line(1 + i), 0.0), axis=1, keepdims=True)
            rows = pl.ds(i * half, half)
            piece = mine[rows, :]
            solved[rows, :] = (dot(full[i], piece, 1, 0) + low * piece.astype(F32)).astype(BF16)

        total[...] = total[...] + dot(mine[...], solved[...], 0, 0)

        for k in range(1, len(pieces) - 2):
            use_cross(k)
        start, count = pieces[-2]
        crosses[-3].wait_recv()
        ready[...] = dot(cross_in[pl.ds(start, count), :], mine[half:, :], 1, 0).astype(BF16)
        crosses[-2].wait_recv()

    @pl.when(jnp.logical_not(below))
    def _():
        ready[...] = jnp.zeros_like(ready)

    for goes, comes, copy in z_copies:
        @pl.when(goes)
        def _():
            copy.wait_send()

    @pl.when(above)
    def _():
        for copy in mixes + crosses:
            copy.wait_send()

    if relay is not None:
        @pl.when(b == via)
        def _():
            second_hop.wait_send()


def finish_kernel(total, mine, tail, ready, out, left, right, held, store_sem):
    late, half = tail.shape
    early = ready.shape[0]
    count = early + late
    width = total.shape[0]
    chunk = TAIL

    kept = jnp.where(lax.axis_index("gy") > 0, tail[...].astype(F32), 0.0).astype(BF16)
    rows = mine[pl.ds(half - count, count), :]
    left[:count, :] = rows
    right[count:, :] = rows
    left[count : count + early, :] = ready[...]
    right[:early, :] = ready[...]
    high = dot(kept, mine[half:, :], 1, 0).astype(BF16)
    left[count + early :, :] = high
    right[early:count, :] = high
    stores = []
    for s in range(width // chunk):
        at = pl.ds(s * chunk, chunk)
        held[at, :] = total[at, :] + dot(left[:, at], right[...], 0, 0)
        store = pltpu.make_async_copy(held.at[at], out.at[0, at], store_sem.at[s])
        store.start()
        stores.append(store)
    for store in stores:
        store.wait()


def in_place(array):
    return pltpu.with_memory_space_constraint(array, pltpu.HBM)


def on_device(relay, factor_inv, sep_sizes, coupling):
    ny, nz = lax.axis_size("gy"), lax.axis_size("gz")
    width = factor_inv.shape[1]
    inter = coupling.shape[2]
    half = width // 2
    block = half // 2
    steps = width // block
    sides = 2 if nz > 2 else 1
    tail = min(TAIL, block)
    pieces = [(start, tail) for start in range(0, half, tail)]
    early = tail - LATE
    pieces = pieces[:-1] + [(half - tail, early), (half - LATE, LATE)]
    count = len(pieces) + 4
    extra = (-(-3 * (half // LANES) // 16) * 16, LANES)
    anywhere = pl.BlockSpec(memory_space=pl.ANY)
    inside = pl.BlockSpec(memory_space=pltpu.VMEM)
    total, mine, last, ready = pl.pallas_call(
        functools.partial(gather_kernel, ny, nz, pieces, relay),
        out_shape=(
            pltpu.VMEM((inter, inter), F32),
            pltpu.VMEM((width, inter), BF16),
            pltpu.VMEM((LATE, half), BF16),
            pltpu.VMEM((early, inter), BF16),
        ),
        in_specs=[pl.BlockSpec(memory_space=pltpu.SMEM), anywhere, anywhere],
        out_specs=(inside,) * 4,
        scratch_shapes=[
            pltpu.VMEM((width, width), BF16),
            pltpu.VMEM((sides, width, inter), BF16),
            pltpu.VMEM((sides, width, width), BF16),
            pltpu.VMEM((width, inter), BF16),
            pltpu.VMEM((half, half), BF16),
            pltpu.VMEM(extra, BF16),
            pltpu.VMEM((half, half), BF16),
            pltpu.VMEM((half, half), BF16),
            pltpu.VMEM(extra, BF16),
            pltpu.VMEM((half, half), BF16),
            pltpu.VMEM((2, half, half), BF16),
            pltpu.VMEM((pieces[RELAYED][1], half), BF16),
            pltpu.SemaphoreType.DMA((7,)),
            pltpu.SemaphoreType.DMA((2,)),
            pltpu.SemaphoreType.DMA((2,)),
            pltpu.SemaphoreType.DMA((count,)),
            pltpu.SemaphoreType.DMA((count,)),
            pltpu.SemaphoreType.DMA((1,)),
            pltpu.SemaphoreType.DMA((1,)),
        ],
        compiler_params=pltpu.CompilerParams(
            collective_id=0, has_side_effects=True, vmem_limit_bytes=40 * 2**20
        ),
    )(sep_sizes, in_place(factor_inv), in_place(coupling))
    return pl.pallas_call(
        finish_kernel,
        out_shape=jax.ShapeDtypeStruct((1, inter, inter), F32),
        in_specs=[inside] * 4,
        out_specs=anywhere,
        scratch_shapes=[
            pltpu.VMEM((2 * tail, inter), BF16),
            pltpu.VMEM((2 * tail, inter), BF16),
            pltpu.VMEM((inter, inter), F32),
            pltpu.SemaphoreType.DMA((inter // TAIL,)),
        ],
        compiler_params=pltpu.CompilerParams(vmem_limit_bytes=40 * 2**20),
    )(total, mine, last, ready)


def relay_of(mesh):
    line = [getattr(mesh.devices[0, b, 0], "coords", None) for b in range(mesh.shape["gy"])]
    if any(at is None for at in line):
        return None
    for b in range(len(line) - 1):
        here, there = line[b], line[b + 1]
        apart = [i for i in range(len(here)) if here[i] != there[i]]
        if len(apart) == 2 and all(abs(here[i] - there[i]) == 1 for i in apart):
            corner = list(here)
            corner[apart[1]] = there[apart[1]]
            if list(corner) in [list(at) for at in line]:
                return b, [list(at) for at in line].index(list(corner))
    return None


def solution(mesh):
    return jax.shard_map(
        functools.partial(on_device, relay_of(mesh)),
        mesh=mesh,
        in_specs=(P("gx", "gy", "gz"), P("gx", "gy", "gz"), P("gx", "gy", "gz")),
        out_specs=P("gx", "gy", "gz"),
        check_vma=False,
    )
```
